32 devices in a mesh: rep: 2 (over z, core), dp: 16 (over x, y).
Axes of the slice: x: 4, y: 4, z: 1, core: 2. Of those that a mesh axis runs over, the one named last changes fastest.
The devices are a block of a 4x4x8 slice.
Arguments:
- g_w_gate: bfloat16 [32, 2, 1280, 4480], P(('rep', 'dp')), parts along dimension 0
- g_w_up: bfloat16 [32, 2, 1280, 4480], P(('rep', 'dp')), parts along dimension 0
- g_w_down: bfloat16 [32, 2, 4480, 1280], P(('rep', 'dp')), parts along dimension 0
- w_gate: bfloat16 [2, 1280, 4480], replicated
- w_up: bfloat16 [2, 1280, 4480], replicated
- w_down: bfloat16 [2, 4480, 1280], replicated
- m_w_gate: float32 [2, 1280, 4480], P(None, 'dp')
- m_w_up: float32 [2, 1280, 4480], P(None, 'dp')
- m_w_down: float32 [2, 4480, 1280], P(None, 'dp')
- v_w_gate: float32 [2, 1280, 4480], P(None, 'dp')
- v_w_up: float32 [2, 1280, 4480], P(None, 'dp')
- v_w_down: float32 [2, 4480, 1280], P(None, 'dp')
Outputs:
- output 1: bfloat16 [4, 1280, 4480], P('rep'), parts along dimension 0
- output 2: bfloat16 [4, 1280, 4480], P('rep'), parts along dimension 0
- output 3: bfloat16 [4, 4480, 1280], P('rep'), parts along dimension 0
- output 4: float32 [4, 1280, 4480], P('rep', 'dp'), parts along dimension 0
- output 5: float32 [4, 1280, 4480], P('rep', 'dp'), parts along dimension 0
- output 6: float32 [4, 4480, 1280], P('rep', 'dp'), parts along dimension 0
- output 7: float32 [4, 1280, 4480], P('rep', 'dp'), parts along dimension 0
- output 8: float32 [4, 1280, 4480], P('rep', 'dp'), parts along dimension 0
- output 9: float32 [4, 4480, 1280], P('rep', 'dp'), parts along dimension 0
There are 2 independent parts. The reference program is written for one: setup_inputs(seed, part) draws one part's arguments, and reference() takes and returns one part's arrays. A program takes and returns all parts, laid end to end along the dimension named above; an argument that names none is the same for every part.
All inputs are finite; a program needn't handle non-finite values.
Results may differ from the reference program's by a relative error of at most 0.022.
Values are sent between devices in bfloat16 or wider.
A program may use at most 768 MiB of HBM per device.

```python
import jax
import jax.numpy as jnp
from jax import lax

DEVICES = 16
D = 1280
FF = 4480
LAYERS = 2
NAMES = ("w_gate", "w_up", "w_down")
SHAPES = {"w_gate": (LAYERS, D, FF), "w_up": (LAYERS, D, FF), "w_down": (LAYERS, FF, D)}


def setup_inputs(seed: int = 0, part: int = 0) -> dict:
    kz, *keys = jax.random.split(jax.random.key(seed), 1 + 5 * len(NAMES))
    loud = 2.0 ** jax.random.uniform(kz, (), jnp.float32, -1.0, 1.0)
    drawn = {}
    for name, key, both in zip(NAMES, keys[:3], keys[3:6], strict=True):
        own = jax.random.normal(jax.random.fold_in(key, part), (DEVICES, *SHAPES[name]), jnp.float32)
        shared = jax.random.normal(jax.random.fold_in(both, part), SHAPES[name], jnp.float32)
        drawn["g_" + name] = (loud * (0.7 * shared / DEVICES + 0.7 * own * DEVICES**-0.5)).astype(jnp.bfloat16)
    for name, key in zip(NAMES, keys[6:9], strict=True):
        drawn[name] = (jax.random.normal(key, SHAPES[name], jnp.float32) * SHAPES[name][1] ** -0.5).astype(jnp.bfloat16)
    for name, key in zip(NAMES, keys[9:12], strict=True):
        drawn["m_" + name] = loud * 0.5 * jax.random.normal(key, SHAPES[name], jnp.float32)
    for name, key in zip(NAMES, keys[12:15], strict=True):
        drawn["v_" + name] = loud * loud * jax.random.uniform(key, SHAPES[name], jnp.float32, 0.5, 1.5)
    return drawn


def adamw(w, m, v, g):
    m = 0.9 * m + 0.1 * g
    v = 0.95 * v + 0.05 * g * g
    step = m * lax.rsqrt(v + 1e-8) + 0.1 * w
    return (w - 0.02 * step).astype(jnp.bfloat16), m, v


def reference(g_w_gate, g_w_up, g_w_down, w_gate, w_up, w_down, m_w_gate, m_w_up, m_w_down, v_w_gate, v_w_up, v_w_down):
    def total(terms):
        return lax.scan(lambda so_far, term: (so_far + term.astype(jnp.float32), None), jnp.zeros(terms.shape[1:], jnp.float32), terms)[0]

    gradients = [total(terms).astype(jnp.bfloat16).astype(jnp.float32) for terms in (g_w_gate, g_w_up, g_w_down)]
    new = [
        adamw(w.astype(jnp.float32), m, v, g)
        for w, m, v, g in zip((w_gate, w_up, w_down), (m_w_gate, m_w_up, m_w_down), (v_w_gate, v_w_up, v_w_down), gradients, strict=True)
    ]
    return tuple(one[which] for which in range(3) for one in new)
```

```python
import functools
import math

import jax
import jax.numpy as jnp
from jax import lax
from jax.experimental import pallas as pl
from jax.experimental.pallas import tpu as pltpu
from jax.sharding import PartitionSpec as P

MESH = pl.DeviceIdType.MESH
RINGS = 4
LANES = 640


def adamw(w, m, v, g):
    m = 0.9 * m + 0.1 * g
    v = 0.95 * v + 0.05 * g * g
    step = m * lax.rsqrt(v + 1e-8) + 0.1 * w
    return (w - 0.02 * step).astype(jnp.bfloat16), m, v


def position(me, cycle, k):
    x, y = me // k, me % k
    return (x if cycle == 0 else y) * k + (x + y) % k


def device(place, cycle, k):
    a, b = place // k, (place % k + k - place // k) % k
    return a * k + b if cycle == 0 else b * k + a


def tiles(rows, columns, body):
    across = columns // LANES
    if across > 1:

        def step(i, _):
            for j in range(across):
                body(pl.ds(pl.multiple_of(i * 8, 8), 8), pl.ds(j * LANES, LANES))
            return 0

        lax.fori_loop(0, rows // 8, step, 0)
    else:
        some = 5 if rows // 8 % 5 == 0 else 1

        def step(i, _):
            for j in range(some):
                body(pl.ds(pl.multiple_of((i * some + j) * 8, 8), 8), pl.ds(0, LANES))
            return 0

        lax.fori_loop(0, rows // 8 // some, step, 0)


def kernel(n, k, g, w, m, v, wo, mo, vo, got, own, ms, vs, ws, sems):
    got_sem, own_sem, send_sem, free_sem, load_sem, store_sem, ag_recv, ag_send, ag_free, keep_sem = sems
    me = lax.axis_index("dp")
    items = [(i, r) for i in range(len(g)) for r in range(RINGS)]
    ways = [1, -1, 1, -1]
    place = [position(me, r // 2, k) for r in range(RINGS)]
    to = [device((place[r] + ways[r] + n) % n, r // 2, k) for r in range(RINGS)]
    back = [device((place[r] - ways[r] + n) % n, r // 2, k) for r in range(RINGS)]

    def split(ref, i, r, block):
        rows, columns = own[i].shape[-2:]
        half = r % 2
        if columns == ref.shape[-1]:
            return ref.at[r // 2, pl.ds(pl.multiple_of(block * 2 * rows + half * rows, 8), rows), :]
        return ref.at[r // 2, pl.ds(pl.multiple_of(block * rows, 8), rows), pl.ds(half * columns, columns)]

    def chunk(ref, i, r, at):
        return split(ref, i, r, device((at + n) % n, r // 2, k))

    def remote(src, dst, send, recv, r):
        return pltpu.make_async_remote_copy(
            src_ref=src, dst_ref=dst, send_sem=send, recv_sem=recv, device_id={"dp": to[r]}, device_id_type=MESH
        )

    def credit(sem, r):
        pl.semaphore_signal(sem, inc=1, device_id={"dp": back[r]}, device_id_type=MESH)

    def load(i, r, s):
        at = place[r] - ways[r] * (1 + s)
        return pltpu.make_async_copy(chunk(g[i].at[0], i, r, at + 2 * n), own[i].at[r, s % 2], own_sem.at[i, r, s % 2])

    def send(i, r, s):
        return remote(own[i].at[r, s % 2], got[i].at[r, s % 2], send_sem.at[i, r, s % 2], got_sem.at[i, r, s % 2], r)

    barrier = pltpu.get_barrier_semaphore()
    for r in range(RINGS):
        pl.semaphore_signal(barrier, inc=1, device_id={"dp": to[r]}, device_id_type=MESH)
    for i, r in items:
        load(i, r, 0).start()
    pl.semaphore_wait(barrier, RINGS)

    for i, r in items:
        load(i, r, 0).wait()
        send(i, r, 0).start()
        load(i, r, 1).start()

    moments = []
    for i, r in items:
        moments += [
            pltpu.make_async_copy(split(ref[i], i, r, 0), buf[i].at[r], load_sem.at[j, i, r])
            for j, (ref, buf) in enumerate(((m, ms), (v, vs)))
        ]
        moments.append(pltpu.make_async_copy(split(w[i], i, r, me), ws[i].at[r], load_sem.at[2, i, r]))
    for one in moments:
        one.start()

    def reduce_step(s, _):
        for i, r in items:
            send(i, r, s - 1).wait_recv()
            load(i, r, s).wait()
            here, there = own[i].at[r, s % 2], got[i].at[r, (s - 1) % 2]

            def add(rows, columns):
                total = here[rows, columns].astype(jnp.float32) + there[rows, columns].astype(jnp.float32)
                here[rows, columns] = total.astype(jnp.bfloat16)

            tiles(*here.shape, add)

            @pl.when(s < n - 2)
            def _():
                credit(free_sem.at[i, r], r)

            @pl.when(s > 1)
            def _():
                pl.semaphore_wait(free_sem.at[i, r], 1)

            send(i, r, s).start()
            send(i, r, s - 1).wait_send()
            load(i, r, s + 1).start()
        return 0

    lax.fori_loop(1, n - 1, reduce_step, 0)

    def part(i, r, t):
        return chunk(wo[i], i, r, place[r] - ways[r] * t + n)

    def forward(i, r, t, src):
        return remote(src, part(i, r, t), ag_send.at[i, r, t % 2], ag_recv.at[i, r, t % 2], r)

    stores = []
    for i, r in items:
        send(i, r, n - 2).wait_recv()
        load(i, r, n - 1).wait()
        here, there = own[i].at[r, (n - 1) % 2], got[i].at[r, (n - 2) % 2]
        for one in moments[3 * (i * RINGS + r) :][:3]:
            one.wait()
        wr, mr, vr = ws[i].at[r], ms[i].at[r], vs[i].at[r]

        def update(rows, columns):
            at = (rows, columns)
            total = (here[at].astype(jnp.float32) + there[at].astype(jnp.float32)).astype(jnp.bfloat16)
            wr[at], mr[at], vr[at] = adamw(wr[at].astype(jnp.float32), mr[at], vr[at], total.astype(jnp.float32))

        tiles(*here.shape, update)
        forward(i, r, 0, wr).start()
        send(i, r, n - 2).wait_send()
        mine = [
            pltpu.make_async_copy(wr, part(i, r, 0), keep_sem.at[i, r]),
            pltpu.make_async_copy(mr, split(mo[i], i, r, 0), store_sem.at[0, i, r]),
            pltpu.make_async_copy(vr, split(vo[i], i, r, 0), store_sem.at[1, i, r]),
        ]
        for one in mine:
            one.start()
        stores += mine

    def gather_step(t, _):
        for i, r in items:
            forward(i, r, t - 1, part(i, r, t)).wait_recv()

            @pl.when(t < n - 2)
            def _():
                credit(ag_free.at[i, r], r)

            @pl.when(t > 1)
            def _():
                pl.semaphore_wait(ag_free.at[i, r], 1)
                forward(i, r, t, part(i, r, t)).wait_send()

            forward(i, r, t, part(i, r, t)).start()
        return 0

    lax.fori_loop(1, n - 1, gather_step, 0)
    for i, r in items:
        forward(i, r, n - 2, part(i, r, n - 1)).wait_recv()
        forward(i, r, n - 3, part(i, r, n - 3)).wait_send()
        forward(i, r, n - 2, part(i, r, n - 2)).wait_send()
    for one in stores:
        one.wait()


def solution(mesh):
    n = mesh.shape["dp"]
    k = math.isqrt(n)

    def step(*arrays):
        g, w, m, v = (arrays[i : i + 3] for i in (0, 3, 6, 9))
        parts = []
        for one in m:
            _, rows, columns = one.shape
            parts.append((rows // 2, columns) if rows // 2 % 8 == 0 else (rows, columns // 2))

        def body(*refs):
            sets = [refs[i : i + 3] for i in range(0, 36, 3)]
            kernel(n, k, *sets, refs[36:])

        any_ = pl.BlockSpec(memory_space=pl.ANY)
        dma, count = pltpu.SemaphoreType.DMA, len(g)
        both, one = (count, RINGS, 2), (count, RINGS)
        shapes = [jax.ShapeDtypeStruct(a.shape, jnp.bfloat16) for a in w]
        shapes += [jax.ShapeDtypeStruct(a.shape, jnp.float32) for a in (*m, *v)]
        scratch = [pltpu.VMEM((RINGS, 2, *p), jnp.bfloat16) for p in parts * 2]
        scratch += [pltpu.VMEM((RINGS, *p), jnp.float32) for p in parts * 2]
        scratch += [pltpu.VMEM((RINGS, *p), jnp.bfloat16) for p in parts]
        scratch += [dma(both), dma(both), dma(both), pltpu.SemaphoreType.REGULAR(one)]
        scratch += [dma((3, *one)), dma((2, *one)), dma(both), dma(both), pltpu.SemaphoreType.REGULAR(one), dma(one)]
        return pl.pallas_call(
            body,
            out_shape=shapes,
            in_specs=[any_] * 12,
            out_specs=[any_] * 9,
            scratch_shapes=scratch,
            compiler_params=pltpu.CompilerParams(
                collective_id=0, has_side_effects=True, vmem_limit_bytes=56 * 2**20
            ),
            name="rings",
        )(*g, *w, *m, *v)

    all_of, cut = P(None, None, None), P(None, "dp", None)
    return jax.shard_map(
        step,
        mesh=mesh,
        in_specs=(P(("rep", "dp"), None, None, None),) * 3 + (all_of,) * 3 + (cut,) * 6,
        out_specs=(P("rep", None, None),) * 3 + (P("rep", "dp", None),) * 6,
        check_vma=False,
    )
```

```python
import functools
import math

import jax
import jax.numpy as jnp
from jax import lax
from jax.experimental import pallas as pl
from jax.experimental.pallas import tpu as pltpu
from jax.sharding import PartitionSpec as P

MESH = pl.DeviceIdType.MESH
RINGS = 4
WAYS = (1, -1, 1, -1)
LANES = 640
HELD = 2
DEPTH = 3


def adamw(w, m, v, g):
    m = 0.9 * m + 0.1 * g
    v = 0.95 * v + 0.05 * g * g
    step = m * lax.rsqrt(v + 1e-8) + 0.1 * w
    return (w - 0.02 * step).astype(jnp.bfloat16), m, v


def position(me, cycle, k):
    x, y = me // k, me % k
    return (x if cycle == 0 else y) * k + (x + y) % k


def device(place, cycle, k):
    a, b = place // k, (place % k + k - place // k) % k
    return a * k + b if cycle == 0 else b * k + a


def tiles(rows, columns, body):
    across = columns // LANES
    if across > 1:

        def step(i, _):
            for j in range(across):
                body(pl.ds(pl.multiple_of(i * 8, 8), 8), pl.ds(j * LANES, LANES))
            return 0

        lax.fori_loop(0, rows // 8, step, 0)
    else:
        some = 5 if rows // 8 % 5 == 0 else 1

        def step(i, _):
            for j in range(some):
                body(pl.ds(pl.multiple_of((i * some + j) * 8, 8), 8), pl.ds(0, LANES))
            return 0

        lax.fori_loop(0, rows // 8 // some, step, 0)


def cut(ref, shape, r, block):
    rows, columns = shape
    half = r % 2
    if columns == ref.shape[-1]:
        return ref.at[r // 2, pl.ds(pl.multiple_of(block * 2 * rows + half * rows, 8), rows), :]
    return ref.at[r // 2, pl.ds(pl.multiple_of(block * rows, 8), rows), pl.ds(half * columns, columns)]


def kernel(n, k, slots, g, w, m, v, wo, mo, vo, out, got, own, ms, vs, ws, sems):
    got_sem, own_sem, send_sem, free_sem, load_sem, store_sem, ag_recv, ag_send, ag_free, keep_sem = sems
    me = lax.axis_index("dp")
    items = [(i, r) for i in range(len(g)) for r in range(RINGS)]
    place = [position(me, r // 2, k) for r in range(RINGS)]
    to = [device((place[r] + WAYS[r] + n) % n, r // 2, k) for r in range(RINGS)]
    back = [device((place[r] - WAYS[r] + n) % n, r // 2, k) for r in range(RINGS)]

    def split(ref, i, r, block):
        return cut(ref, own[i].shape[-2:], r, block)

    def chunk(ref, i, r, at):
        return split(ref, i, r, device((at + n) % n, r // 2, k))

    def remote(src, dst, send, recv, r):
        return pltpu.make_async_remote_copy(
            src_ref=src, dst_ref=dst, send_sem=send, recv_sem=recv, device_id={"dp": to[r]}, device_id_type=MESH
        )

    def credit(sem, r):
        pl.semaphore_signal(sem, inc=1, device_id={"dp": back[r]}, device_id_type=MESH)

    def load(i, r, s):
        at = place[r] - WAYS[r] * (1 + s)
        return pltpu.make_async_copy(chunk(g[i].at[0], i, r, at + 2 * n), own[i].at[r, s % 2], own_sem.at[i, r, s % 2])

    def send(i, r, s):
        return remote(own[i].at[r, s % 2], got[i].at[r, s % 2], send_sem.at[i, r, s % 2], got_sem.at[i, r, s % 2], r)

    barrier = pltpu.get_barrier_semaphore()
    for r in range(RINGS):
        pl.semaphore_signal(barrier, inc=1, device_id={"dp": to[r]}, device_id_type=MESH)
    for i, r in items:
        load(i, r, 0).start()
    pl.semaphore_wait(barrier, RINGS)

    for i, r in items:
        load(i, r, 0).wait()
        send(i, r, 0).start()
        load(i, r, 1).start()

    moments = []
    for i, r in items:
        moments += [
            pltpu.make_async_copy(split(ref[i], i, r, 0), buf[i].at[r], load_sem.at[j, i, r])
            for j, (ref, buf) in enumerate(((m, ms), (v, vs)))
        ]
        moments.append(pltpu.make_async_copy(split(w[i], i, r, me), ws[i].at[r], load_sem.at[2, i, r]))
    for one in moments:
        one.start()

    def reduce_step(s, _):
        for i, r in items:
            send(i, r, s - 1).wait_recv()
            load(i, r, s).wait()
            here, there = own[i].at[r, s % 2], got[i].at[r, (s - 1) % 2]

            def add(rows, columns):
                total = here[rows, columns].astype(jnp.float32) + there[rows, columns].astype(jnp.float32)
                here[rows, columns] = total.astype(jnp.bfloat16)

            tiles(*here.shape, add)

            @pl.when(s < n - 2)
            def _():
                credit(free_sem.at[i, r], r)

            @pl.when(s > 1)
            def _():
                pl.semaphore_wait(free_sem.at[i, r], 1)

            send(i, r, s).start()
            send(i, r, s - 1).wait_send()
            load(i, r, s + 1).start()
        return 0

    lax.fori_loop(1, n - 1, reduce_step, 0)

    def part(i, r, t):
        return chunk(wo[i], i, r, place[r] - WAYS[r] * t + n)

    def forward(i, r, t, src, dst=None):
        dst = part(i, r, t) if dst is None else dst
        return remote(src, dst, ag_send.at[i, r, t % 2], ag_recv.at[i, r, t % 2], r)

    def passed(i, r, which):
        group, slot = slots[i]
        return out[r][group].at[which, slot]

    stores = []
    for i, r in items:
        send(i, r, n - 2).wait_recv()
        load(i, r, n - 1).wait()
        here, there = own[i].at[r, (n - 1) % 2], got[i].at[r, (n - 2) % 2]
        for one in moments[3 * (i * RINGS + r) :][:3]:
            one.wait()
        wr, mr, vr = ws[i].at[r], ms[i].at[r], vs[i].at[r]

        def update(rows, columns):
            at = (rows, columns)
            total = (here[at].astype(jnp.float32) + there[at].astype(jnp.float32)).astype(jnp.bfloat16)
            wr[at], mr[at], vr[at] = adamw(wr[at].astype(jnp.float32), mr[at], vr[at], total.astype(jnp.float32))

        tiles(*here.shape, update)
        forward(i, r, 0, wr).start()
        send(i, r, n - 2).wait_send()
        mine = [
            pltpu.make_async_copy(wr, passed(i, r ^ 1, 1), keep_sem.at[i, r]),
            pltpu.make_async_copy(mr, split(mo[i], i, r, 0), store_sem.at[0, i, r]),
            pltpu.make_async_copy(vr, split(vo[i], i, r, 0), store_sem.at[1, i, r]),
        ]
        for one in mine:
            one.start()
        stores += mine

    end = n - HELD - 2

    def gather_step(t, _):
        for i, r in items:
            forward(i, r, t - 1, part(i, r, t)).wait_recv()

            credit(ag_free.at[i, r], r)

            @pl.when(t > 1)
            def _():
                pl.semaphore_wait(ag_free.at[i, r], 1)
                forward(i, r, t, part(i, r, t)).wait_send()

            forward(i, r, t, part(i, r, t)).start()
        return 0

    lax.fori_loop(1, end, gather_step, 0)
    for i, r in items:
        forward(i, r, end - 1, part(i, r, end)).wait_recv()
        pl.semaphore_wait(ag_free.at[i, r], 1)
        forward(i, r, end - 2, part(i, r, end - 2)).wait_send()
        forward(i, r, end, part(i, r, end), passed(i, r, 0)).start()
    for i, r in items:
        forward(i, r, end, part(i, r, end), passed(i, r, 0)).wait_recv()
        forward(i, r, end - 1, part(i, r, end - 1)).wait_send()
        forward(i, r, end, part(i, r, end), passed(i, r, 0)).wait_send()
    for one in stores:
        one.wait()


def spread(n, k, slots, wc, out, m, v, wo, mo, vo, buf, ms, vs, sems):
    read_sem, write_sem, in_sem, back_sem = sems
    me = lax.axis_index("dp")
    place = [position(me, r // 2, k) for r in range(RINGS)]
    items = [(i, r) for i in range(len(wc)) for r in range(RINGS)]
    last = n - HELD - 1

    def part(ref, i, r, t):
        return cut(ref, buf[i].shape[-2:], r, device((place[r] - WAYS[r] * t + n) % n, r // 2, k))

    def read(i, r, t, which=None):
        group, slot = slots[i]
        at = part(wc[i], i, r, t) if which is None else out[r ^ which][group].at[which, slot]
        return pltpu.make_async_copy(at, buf[i].at[r, t % DEPTH], read_sem.at[i, r, t % DEPTH])

    def write(i, r, t):
        return pltpu.make_async_copy(buf[i].at[r, t % DEPTH], part(wo[i], i, r, t), write_sem.at[i, r, t % DEPTH])

    def turn(t, which=None, first=False):
        for i, r in items:
            if not first:
                write(i, r, t - DEPTH).wait()
            read(i, r, t, which).start()
        for i, r in items:
            read(i, r, t - 1).wait()
            write(i, r, t - 1).start()
        return 0

    moments = []
    for j, (source, scratch, target) in enumerate(((m, ms, mo), (v, vs, vo))):
        for i in range(len(source)):
            one = pltpu.make_async_copy(source[i], scratch[i], in_sem.at[j, i])
            moments.append((one, pltpu.make_async_copy(scratch[i], target[i], back_sem.at[j, i])))
    for i, r in items:
        read(i, r, 0, 1).start()
    for one, _ in moments:
        one.start()
    turn(1, first=True)
    turn(2, first=True)
    for one, other in moments:
        one.wait()
        other.start()
    lax.fori_loop(DEPTH, last, lambda t, _: turn(t), 0)
    turn(last, 0)
    for i, r in items:
        read(i, r, last, 0).wait()
        write(i, r, last).start()
    for t in range(last - DEPTH + 1, last + 1):
        for i, r in items:
            write(i, r, t).wait()
    for _, other in moments:
        other.wait()


def fill(n, k, slots, got, wo, buf, read_sem, write_sem):
    me = lax.axis_index("dp")
    place = [position(me, r // 2, k) for r in range(RINGS)]
    pieces = [(r, group) for group in range(len(buf)) for r in range(RINGS)]
    reads = [pltpu.make_async_copy(got[r][group], buf[group].at[r], read_sem.at[r, group]) for r, group in pieces]
    for one in reads:
        one.start()
    writes = []
    for one, (r, group) in zip(reads, pieces, strict=True):
        one.wait()
        for i, (its, slot) in enumerate(slots):
            if its != group:
                continue
            for which, at in enumerate((place[r] + WAYS[r] * HELD, place[r] - WAYS[r])):
                target = cut(wo[i], buf[group].shape[-2:], r ^ which, device((at + n) % n, r // 2, k))
                writes.append(pltpu.make_async_copy(buf[group].at[r, which, slot], target, write_sem.at[r, which, i]))
                writes[-1].start()
    for one in writes:
        one.wait()


def solution(mesh):
    n = mesh.shape["dp"]
    k = math.isqrt(n)
    routes = []
    for r in range(RINGS):
        routes.append([(device(p, r // 2, k), device((p + WAYS[r]) % n, r // 2, k)) for p in range(n)])

    def step(*arrays):
        g, w, m, v = (arrays[i : i + 3] for i in (0, 3, 6, 9))
        count, bf16, f32 = len(g), jnp.bfloat16, jnp.float32
        parts = []
        for one in m:
            _, rows, columns = one.shape
            parts.append((rows // 2, columns) if rows // 2 % 8 == 0 else (rows, columns // 2))
        kinds = sorted(set(parts))
        slots = [(kinds.index(p), parts[:i].count(p)) for i, p in enumerate(parts)]
        sizes = [(2, parts.count(p), *p) for p in kinds]
        groups = len(kinds)

        any_ = pl.BlockSpec(memory_space=pl.ANY)
        dma, count_sem = pltpu.SemaphoreType.DMA, pltpu.SemaphoreType.REGULAR
        both, one = (count, RINGS, 2), (count, RINGS)

        def threes(refs):
            return [refs[i : i + count] for i in range(0, len(refs), count)]

        def by_ring(refs):
            return [refs[i : i + groups] for i in range(0, len(refs), groups)]

        def rings(*refs):
            ahead, out, behind = refs[: 7 * count], refs[7 * count :][: RINGS * groups], refs[7 * count + RINGS * groups :]
            kernel(n, k, slots, *threes(ahead), by_ring(out), *threes(behind[: 5 * count]), behind[5 * count :])

        whole = [jax.ShapeDtypeStruct(a.shape, bf16) for a in w]
        kept = [jax.ShapeDtypeStruct(a.shape, f32) for a in (*m, *v)]
        passed = [jax.ShapeDtypeStruct(s, bf16) for _ in range(RINGS) for s in sizes]
        scratch = [pltpu.VMEM((RINGS, 2, *p), bf16) for p in parts * 2]
        scratch += [pltpu.VMEM((RINGS, *p), f32) for p in parts * 2]
        scratch += [pltpu.VMEM((RINGS, *p), bf16) for p in parts]
        scratch += [dma(both), dma(both), dma(both), count_sem(one)]
        scratch += [dma((3, *one)), dma((2, *one)), dma(both), dma(both), count_sem(one), dma(one)]
        made = pl.pallas_call(
            rings,
            out_shape=whole + kept + passed,
            in_specs=[any_] * (4 * count),
            out_specs=[any_] * (3 * count + RINGS * groups),
            scratch_shapes=scratch,
            compiler_params=pltpu.CompilerParams(
                collective_id=0, has_side_effects=True, vmem_limit_bytes=56 * 2**20
            ),
            name="rings",
        )(*g, *w, *m, *v)
        wc, moments, out = made[:count], made[count : 3 * count], made[3 * count :]
        hops = [lax.ppermute(a, "dp", routes[j // groups]) for j, a in enumerate(out)]

        def copies(*refs):
            ends = [count, RINGS * groups, *[count] * 5, *[count] * 3]
            sets, at = [], 0
            for size in ends:
                sets.append(refs[at : at + size])
                at += size
            sets[1] = by_ring(sets[1])
            spread(n, k, slots, *sets, refs[at:])

        deep = (count, RINGS, DEPTH)
        final = pl.pallas_call(
            copies,
            out_shape=whole + kept,
            in_specs=[any_] * (3 * count + RINGS * groups),
            out_specs=[any_] * (3 * count),
            scratch_shapes=[pltpu.VMEM((RINGS, DEPTH, *p), bf16) for p in parts]
            + [pltpu.VMEM(a.shape, f32) for a in (*m, *v)]
            + [dma(deep), dma(deep), dma((2, count)), dma((2, count))],
            compiler_params=pltpu.CompilerParams(vmem_limit_bytes=48 * 2**20),
            cost_estimate=pl.CostEstimate(flops=10**9, bytes_accessed=170 * 10**6, transcendentals=0),
            name="spread",
        )(*wc, *out, *moments)

        def puts(*refs):
            got, wo = by_ring(refs[: RINGS * groups]), refs[RINGS * groups + count :][:count]
            rest = refs[RINGS * groups + 2 * count :]
            fill(n, k, slots, got, wo, rest[:groups], *rest[groups:])

        new = pl.pallas_call(
            puts,
            out_shape=whole,
            in_specs=[any_] * (RINGS * groups + count),
            out_specs=[any_] * count,
            input_output_aliases={RINGS * groups + i: i for i in range(count)},
            scratch_shapes=[pltpu.VMEM((RINGS, *s), bf16) for s in sizes] + [dma((RINGS, groups)), dma((RINGS, 2, count))],
            compiler_params=pltpu.CompilerParams(vmem_limit_bytes=24 * 2**20),
            cost_estimate=pl.CostEstimate(flops=10**8, bytes_accessed=17 * 10**6, transcendentals=0),
            name="fill",
        )(*hops, *final[:count])
        return (*new, *final[count:])

    all_of, own = P(None, None, None), P(None, "dp", None)
    return jax.shard_map(
        step,
        mesh=mesh,
        in_specs=(P(("rep", "dp"), None, None, None),) * 3 + (all_of,) * 3 + (own,) * 6,
        out_specs=(P("rep", None, None),) * 3 + (P("rep", "dp", None),) * 6,
        check_vma=False,
    )
```

```python
import functools
import math

import jax
import jax.numpy as jnp
from jax import lax
from jax.experimental import pallas as pl
from jax.experimental.pallas import tpu as pltpu
from jax.sharding import PartitionSpec as P

MESH = pl.DeviceIdType.MESH
RINGS = 4
WAYS = (1, -1, 1, -1)
LANES = 640
HELD = 2
DEPTH = 2


def adamw(w, m, v, g):
    m = 0.9 * m + 0.1 * g
    v = 0.95 * v + 0.05 * g * g
    step = m * lax.rsqrt(v + 1e-8) + 0.1 * w
    return (w - 0.02 * step).astype(jnp.bfloat16), m, v


def position(me, cycle, k):
    x, y = me // k, me % k
    return (x if cycle == 0 else y) * k + (x + y) % k


def device(place, cycle, k):
    a, b = place // k, (place % k + k - place // k) % k
    return a * k + b if cycle == 0 else b * k + a


def tiles(rows, columns, body):
    across = columns // LANES
    if across > 1:

        def step(i, _):
            for j in range(across):
                body(pl.ds(pl.multiple_of(i * 8, 8), 8), pl.ds(j * LANES, LANES))
            return 0

        lax.fori_loop(0, rows // 8, step, 0)
    else:
        some = 5 if rows // 8 % 5 == 0 else 1

        def step(i, _):
            for j in range(some):
                body(pl.ds(pl.multiple_of((i * some + j) * 8, 8), 8), pl.ds(0, LANES))
            return 0

        lax.fori_loop(0, rows // 8 // some, step, 0)


def cut(ref, shape, r, block):
    rows, columns = shape
    half = r % 2
    if columns == ref.shape[-1]:
        return ref.at[r // 2, pl.ds(pl.multiple_of(block * 2 * rows + half * rows, 8), rows), :]
    return ref.at[r // 2, pl.ds(pl.multiple_of(block * rows, 8), rows), pl.ds(half * columns, columns)]


def passed(out, slots, i, r, which):
    group, slot = slots[i]
    return out[r][group].at[which, slot]


def kept(out, got, own, slots, i, r, t, last):
    if t == 0:
        return passed(out, slots, i, r ^ 1, 1)
    if t == last:
        return passed(out, slots, i, r, 0)
    return (own if t > last - 3 else got)[i].at[r, t % 2]


def kernel(n, k, slots, g, w, m, v, wo, mo, vo, out, got, own, sems):
    got_sem, own_sem, send_sem, free_sem, load_sem, ag_recv, ag_send, ag_free = sems
    me = lax.axis_index("dp")
    items = [(i, r) for i in range(len(g)) for r in range(RINGS)]
    place = [position(me, r // 2, k) for r in range(RINGS)]
    to = [device((place[r] + WAYS[r] + n) % n, r // 2, k) for r in range(RINGS)]
    back = [device((place[r] - WAYS[r] + n) % n, r // 2, k) for r in range(RINGS)]

    def split(ref, i, r, block):
        return cut(ref, own[i].shape[-2:], r, block)

    def chunk(ref, i, r, at):
        return split(ref, i, r, device((at + n) % n, r // 2, k))

    def remote(src, dst, send, recv, r):
        return pltpu.make_async_remote_copy(
            src_ref=src, dst_ref=dst, send_sem=send, recv_sem=recv, device_id={"dp": to[r]}, device_id_type=MESH
        )

    def credit(sem, r):
        pl.semaphore_signal(sem, inc=1, device_id={"dp": back[r]}, device_id_type=MESH)

    def load(i, r, s):
        at = place[r] - WAYS[r] * (1 + s)
        return pltpu.make_async_copy(chunk(g[i].at[0], i, r, at + 2 * n), own[i].at[r, s % 2], own_sem.at[i, r, s % 2])

    def send(i, r, s):
        return remote(own[i].at[r, s % 2], got[i].at[r, s % 2], send_sem.at[i, r, s % 2], got_sem.at[i, r, s % 2], r)

    barrier = pltpu.get_barrier_semaphore()
    for r in range(RINGS):
        pl.semaphore_signal(barrier, inc=1, device_id={"dp": to[r]}, device_id_type=MESH)
    for i, r in items:
        load(i, r, 0).start()
    pl.semaphore_wait(barrier, RINGS)

    for i, r in items:
        load(i, r, 0).wait()
        send(i, r, 0).start()
        load(i, r, 1).start()

    state = []
    for i, r in items:
        pairs = [(split(m[i], i, r, 0), split(mo[i], i, r, 0)), (split(v[i], i, r, 0), split(vo[i], i, r, 0))]
        pairs.append((split(w[i], i, r, me), passed(out, slots, i, r ^ 1, 1)))
        state.append([pltpu.make_async_copy(*pair, load_sem.at[j, i, r]) for j, pair in enumerate(pairs)])
    for one in state:
        for copy in one:
            copy.start()

    def reduce_step(s, _):
        for i, r in items:
            send(i, r, s - 1).wait_recv()
            load(i, r, s).wait()
            here, there = own[i].at[r, s % 2], got[i].at[r, (s - 1) % 2]

            def add(rows, columns):
                total = here[rows, columns].astype(jnp.float32) + there[rows, columns].astype(jnp.float32)
                here[rows, columns] = total.astype(jnp.bfloat16)

            tiles(*here.shape, add)

            @pl.when(s < n - 2)
            def _():
                credit(free_sem.at[i, r], r)

            @pl.when(s > 1)
            def _():
                pl.semaphore_wait(free_sem.at[i, r], 1)

            send(i, r, s).start()
            send(i, r, s - 1).wait_send()
            load(i, r, s + 1).start()
        return 0

    lax.fori_loop(1, n - 1, reduce_step, 0)

    last = n - HELD - 1
    near = last - 5

    def at(i, r, t):
        if isinstance(t, int) and not 1 <= t <= near:
            return kept(out, got, own, slots, i, r, t, last)
        return chunk(wo[i], i, r, place[r] - WAYS[r] * t + n)

    def after(i, r, t):
        if isinstance(t, int) and t >= near:
            return kept(out, got, own, slots, i, r, t + 1, last)
        return chunk(wo[i], i, r, place[r] - WAYS[r] * t + n)

    def forward(i, r, t):
        return remote(at(i, r, t), after(i, r, t), ag_send.at[i, r, t % 2], ag_recv.at[i, r, t % 2], r)

    for i, r in items:
        send(i, r, n - 2).wait_recv()
        load(i, r, n - 1).wait()
        here, there = own[i].at[r, (n - 1) % 2], got[i].at[r, (n - 2) % 2]
        for copy in state[i * RINGS + r]:
            copy.wait()
        wr, mr, vr = passed(out, slots, i, r ^ 1, 1), split(mo[i], i, r, 0), split(vo[i], i, r, 0)

        def update(rows, columns):
            at = (rows, columns)
            total = (here[at].astype(jnp.float32) + there[at].astype(jnp.float32)).astype(jnp.bfloat16)
            wr[at], mr[at], vr[at] = adamw(wr[at].astype(jnp.float32), mr[at], vr[at], total.astype(jnp.float32))

        tiles(*here.shape, update)
        forward(i, r, 0).start()
        send(i, r, n - 2).wait_send()

    def gather_step(t, credited=True):
        for i, r in items:
            forward(i, r, t - 1).wait_recv()
            if credited:
                credit(ag_free.at[i, r], r)

            @pl.when(t > 1)
            def _():
                pl.semaphore_wait(ag_free.at[i, r], 1)
                forward(i, r, t - 2).wait_send()

            forward(i, r, t).start()
        return 0

    lax.fori_loop(1, near, lambda t, _: gather_step(t), 0)
    for t in range(near, last):
        gather_step(t, credited=t < last - 1)
    for i, r in items:
        forward(i, r, last - 1).wait_recv()
        forward(i, r, last - 2).wait_send()
        forward(i, r, last - 1).wait_send()


def spread(n, k, slots, wc, out, got, own, m, v, wo, mo, vo, buf, sems):
    read_sem, write_sem, kept_sem, back_sem = sems
    me = lax.axis_index("dp")
    place = [position(me, r // 2, k) for r in range(RINGS)]
    items = [(i, r) for i in range(len(wc)) for r in range(RINGS)]
    last = n - HELD - 1
    near = last - 5

    def part(ref, i, r, t):
        return cut(ref, buf[i].shape[-2:], r, device((place[r] - WAYS[r] * t + n) % n, r // 2, k))

    def read(i, r, t):
        return pltpu.make_async_copy(part(wc[i], i, r, t), buf[i].at[r, t % DEPTH], read_sem.at[i, r, t % DEPTH])

    def write(i, r, t):
        return pltpu.make_async_copy(buf[i].at[r, t % DEPTH], part(wo[i], i, r, t), write_sem.at[i, r, t % DEPTH])

    straight = []
    for j, t in enumerate((0, *range(near + 1, last + 1))):
        for i, r in items:
            chunk = kept(out, got, own, slots, i, r, t, last)
            straight.append(pltpu.make_async_copy(chunk, part(wo[i], i, r, t), kept_sem.at[j, i, r]))
    for j, (source, target) in enumerate(((m, mo), (v, vo))):
        straight += [pltpu.make_async_copy(source[i], target[i], back_sem.at[j, i]) for i in range(len(source))]
    each = -(-len(straight) // near)

    for t in range(1, near + 2):
        if t <= near:
            for i, r in items:
                if t > DEPTH:
                    write(i, r, t - DEPTH).wait()
                read(i, r, t).start()
            for copy in straight[(t - 1) * each : t * each]:
                copy.start()
        if t > 1:
            for i, r in items:
                read(i, r, t - 1).wait()
                write(i, r, t - 1).start()
    for t in range(near - DEPTH + 1, near + 1):
        for i, r in items:
            write(i, r, t).wait()
    for copy in straight:
        copy.wait()


def fill(n, k, part, hops, wo, sem):
    me = lax.axis_index("dp")
    place = [position(me, r // 2, k) for r in range(RINGS)]
    writes = []
    for slot, ref in enumerate(wo):
        for r in range(RINGS):
            for which, at in enumerate((place[r] + WAYS[r] * HELD, place[r] - WAYS[r])):
                target = cut(ref, part, r ^ which, device((at + n) % n, r // 2, k))
                writes.append(pltpu.make_async_copy(hops[r].at[which, slot], target, sem.at[slot, r, which]))
    for one in writes:
        one.start()
    for one in writes:
        one.wait()


def sets(refs, *sizes):
    found, at = [], 0
    for size in sizes:
        found.append(refs[at : at + size])
        at += size
    return *found, refs[at:]


def solution(mesh):
    n = mesh.shape["dp"]
    k = math.isqrt(n)
    routes = []
    for r in range(RINGS):
        routes.append([(device(p, r // 2, k), device((p + WAYS[r]) % n, r // 2, k)) for p in range(n)])

    def step(*arrays):
        g, w, m, v = (arrays[i : i + 3] for i in (0, 3, 6, 9))
        count, bf16, f32 = len(g), jnp.bfloat16, jnp.float32
        parts = []
        for one in m:
            _, rows, columns = one.shape
            parts.append((rows // 2, columns) if rows // 2 % 8 == 0 else (rows, columns // 2))
        kinds = sorted(set(parts))
        slots = [(kinds.index(p), parts[:i].count(p)) for i, p in enumerate(parts)]
        groups = len(kinds)
        many = RINGS * groups

        hbm, vmem = pl.BlockSpec(memory_space=pl.ANY), pl.BlockSpec(memory_space=pltpu.VMEM)
        dma, plain = pltpu.SemaphoreType.DMA, pltpu.SemaphoreType.REGULAR
        both, one = (count, RINGS, 2), (count, RINGS)

        def by_ring(refs):
            return [refs[i : i + groups] for i in range(0, len(refs), groups)]

        def placed(values, space):
            return [pltpu.with_memory_space_constraint(a, space) for a in values]

        def rings(*refs):
            *ahead, out, got, own, sems = sets(refs, *[count] * 7, many, count, count)
            kernel(n, k, slots, *ahead, by_ring(out), got, own, sems)

        whole = [jax.ShapeDtypeStruct(a.shape, bf16) for a in w]
        moments = [pltpu.VMEM(a.shape, f32) for a in (*m, *v)]
        passing = [pltpu.VMEM((2, parts.count(p), *p), bf16) for _ in range(RINGS) for p in kinds]
        buffers = [pltpu.VMEM((RINGS, 2, *p), bf16) for p in parts * 2]
        made = pl.pallas_call(
            rings,
            out_shape=whole + moments + passing + buffers,
            in_specs=[hbm] * (4 * count),
            out_specs=[hbm] * count + [vmem] * (4 * count + many),
            scratch_shapes=[dma(both), dma(both), dma(both), plain(one), dma((3, *one)), dma(both), dma(both), plain(one)],
            compiler_params=pltpu.CompilerParams(
                collective_id=0, has_side_effects=True, vmem_limit_bytes=4 * 2**20
            ),
            name="rings",
        )(*placed((*g, *w, *m, *v), pltpu.HBM))
        gathered, moved, out, kept_here, _ = sets(made, count, 2 * count, many, 2 * count)
        hops = [lax.ppermute(a, "dp", routes[j // groups]) for j, a in enumerate(out)]

        def copies(*refs):
            wc, out, got, own, ms, vs, wo, mo, vo, buf, sems = sets(refs, count, many, *[count] * 8)
            spread(n, k, slots, wc, by_ring(out), got, own, ms, vs, wo, mo, vo, buf, sems)

        deep = (count, RINGS, DEPTH)
        final = pl.pallas_call(
            copies,
            out_shape=whole + [jax.ShapeDtypeStruct(a.shape, f32) for a in (*m, *v)],
            in_specs=[hbm] * count + [vmem] * (4 * count + many),
            out_specs=[hbm] * (3 * count),
            scratch_shapes=[pltpu.VMEM((RINGS, DEPTH, *p), bf16) for p in parts]
            + [dma(deep), dma(deep), dma((6, *one)), dma((2, count))],
            compiler_params=pltpu.CompilerParams(vmem_limit_bytes=9 * 2**20),
            cost_estimate=pl.CostEstimate(flops=10**9, bytes_accessed=112 * 10**6, transcendentals=0),
            name="spread",
        )(*gathered, *placed((*out, *kept_here, *moved), pltpu.VMEM))

        new, before = list(final[:count]), []
        for group, part in enumerate(kinds):
            its = [i for i, (one, _) in enumerate(slots) if one == group]

            def puts(*refs, part=part, size=len(its)):
                hops, _, wo, (sem,) = sets(refs, RINGS, len(refs) - RINGS - size - 1, size)
                fill(n, k, part, hops, wo, sem)

            filled = pl.pallas_call(
                puts,
                out_shape=[whole[i] for i in its],
                in_specs=[vmem] * RINGS + [hbm] * (len(its) + len(before)),
                out_specs=[hbm] * len(its),
                input_output_aliases={RINGS + j: j for j in range(len(its))},
                scratch_shapes=[dma((len(its), RINGS, 2))],
                compiler_params=pltpu.CompilerParams(vmem_limit_bytes=2 * 2**20),
                cost_estimate=pl.CostEstimate(flops=10**8, bytes_accessed=9 * 10**6, transcendentals=0),
                name=f"fill_{group}",
            )(*placed(hops[group::groups], pltpu.VMEM), *placed([*[final[i] for i in its], *before], pltpu.HBM))
            for i, one in zip(its, filled, strict=True):
                new[i] = one
            before = filled
        return (*new, *final[count:])

    all_of, block = P(None, None, None), P(None, "dp", None)
    return jax.shard_map(
        step,
        mesh=mesh,
        in_specs=(P(("rep", "dp"), None, None, None),) * 3 + (all_of,) * 3 + (block,) * 6,
        out_specs=(P("rep", None, None),) * 3 + (P("rep", "dp", None),) * 6,
        check_vma=False,
    )
```

```python
import functools
import math

import jax
import jax.numpy as jnp
from jax import lax
from jax.experimental import pallas as pl
from jax.experimental.pallas import tpu as pltpu
from jax.sharding import PartitionSpec as P

MESH = pl.DeviceIdType.MESH
RINGS = 4
WAYS = (1, -1, 1, -1)
LANES = 640
HELD = 2
DEPTH = 2


def adamw(w, m, v, g):
    m = 0.9 * m + 0.1 * g
    v = 0.95 * v + 0.05 * g * g
    step = m * lax.rsqrt(v + 1e-8) + 0.1 * w
    return (w - 0.02 * step).astype(jnp.bfloat16), m, v


def position(me, cycle, k):
    x, y = me // k, me % k
    return (x if cycle == 0 else y) * k + (x + y) % k


def device(place, cycle, k):
    a, b = place // k, (place % k + k - place // k) % k
    return a * k + b if cycle == 0 else b * k + a


def tiles(rows, columns, body):
    across = columns // LANES
    if across > 1:

        def step(i, _):
            for j in range(across):
                body(pl.ds(pl.multiple_of(i * 8, 8), 8), pl.ds(j * LANES, LANES))
            return 0

        lax.fori_loop(0, rows // 8, step, 0)
    else:
        some = 5 if rows // 8 % 5 == 0 else 1

        def step(i, _):
            for j in range(some):
                body(pl.ds(pl.multiple_of((i * some + j) * 8, 8), 8), pl.ds(0, LANES))
            return 0

        lax.fori_loop(0, rows // 8 // some, step, 0)


def cut(ref, shape, r, block):
    rows, columns = shape
    half = r % 2
    if columns == ref.shape[-1]:
        return ref.at[r // 2, pl.ds(pl.multiple_of(block * 2 * rows + half * rows, 8), rows), :]
    return ref.at[r // 2, pl.ds(pl.multiple_of(block * rows, 8), rows), pl.ds(half * columns, columns)]


def passed(out, slots, i, r, which):
    group, slot = slots[i]
    return out[r][group].at[which, slot]


def kept(out, got, own, slots, i, r, t, last):
    if t == 0:
        return passed(out, slots, i, r ^ 1, 1)
    if t == last:
        return passed(out, slots, i, r, 0)
    return (own if t > last - 3 else got)[i].at[r, t % 2]


def kernel(n, k, slots, g, w, m, v, wo, mo, vo, out, got, own, sems):
    got_sem, own_sem, send_sem, free_sem, load_sem, ag_recv, ag_send, ag_free = sems
    me = lax.axis_index("dp")
    items = [(i, r) for i in range(len(g)) for r in range(RINGS)]
    place = [position(me, r // 2, k) for r in range(RINGS)]
    to = [device((place[r] + WAYS[r] + n) % n, r // 2, k) for r in range(RINGS)]
    back = [device((place[r] - WAYS[r] + n) % n, r // 2, k) for r in range(RINGS)]

    def split(ref, i, r, block):
        return cut(ref, own[i].shape[-2:], r, block)

    def chunk(ref, i, r, at):
        return split(ref, i, r, device((at + n) % n, r // 2, k))

    def remote(src, dst, send, recv, r):
        return pltpu.make_async_remote_copy(
            src_ref=src, dst_ref=dst, send_sem=send, recv_sem=recv, device_id={"dp": to[r]}, device_id_type=MESH
        )

    def credit(sem, r):
        pl.semaphore_signal(sem, inc=1, device_id={"dp": back[r]}, device_id_type=MESH)

    def load(i, r, s):
        at = place[r] - WAYS[r] * (1 + s)
        return pltpu.make_async_copy(chunk(g[i].at[0], i, r, at + 2 * n), own[i].at[r, s % 2], own_sem.at[i, r, s % 2])

    def first(i, r):
        term = chunk(g[i].at[0], i, r, place[r] - WAYS[r] + n)
        return remote(term, got[i].at[r, 0], send_sem.at[i, r, 0], got_sem.at[i, r, 0], r)

    def send(i, r, s):
        return remote(own[i].at[r, s % 2], got[i].at[r, s % 2], send_sem.at[i, r, s % 2], got_sem.at[i, r, s % 2], r)

    barrier = pltpu.get_barrier_semaphore()
    for r in range(RINGS):
        pl.semaphore_signal(barrier, inc=1, device_id={"dp": to[r]}, device_id_type=MESH)
    for i, r in items:
        load(i, r, 1).start()
    pl.semaphore_wait(barrier, RINGS)

    for i, r in items:
        first(i, r).start()

    state = []
    for i, r in items:
        pairs = [(split(m[i], i, r, 0), split(mo[i], i, r, 0)), (split(v[i], i, r, 0), split(vo[i], i, r, 0))]
        pairs.append((split(w[i], i, r, me), passed(out, slots, i, r ^ 1, 1)))
        state.append([pltpu.make_async_copy(*pair, load_sem.at[j, i, r]) for j, pair in enumerate(pairs)])
    for one in state:
        for copy in one:
            copy.start()

    def reduce_step(s, _):
        for i, r in items:
            send(i, r, s - 1).wait_recv()
            load(i, r, s).wait()
            here, there = own[i].at[r, s % 2], got[i].at[r, (s - 1) % 2]

            def add(rows, columns):
                total = here[rows, columns].astype(jnp.float32) + there[rows, columns].astype(jnp.float32)
                here[rows, columns] = total.astype(jnp.bfloat16)

            tiles(*here.shape, add)

            @pl.when(s < n - 2)
            def _():
                credit(free_sem.at[i, r], r)

            @pl.when(s > 1)
            def _():
                pl.semaphore_wait(free_sem.at[i, r], 1)

            send(i, r, s).start()
            send(i, r, s - 1).wait_send()
            load(i, r, s + 1).start()
        return 0

    lax.fori_loop(1, n - 1, reduce_step, 0)

    last = n - HELD - 1
    near = last - 5

    def at(i, r, t):
        if isinstance(t, int) and not 1 <= t <= near:
            return kept(out, got, own, slots, i, r, t, last)
        return chunk(wo[i], i, r, place[r] - WAYS[r] * t + n)

    def after(i, r, t):
        if isinstance(t, int) and t >= near:
            return kept(out, got, own, slots, i, r, t + 1, last)
        return chunk(wo[i], i, r, place[r] - WAYS[r] * t + n)

    def forward(i, r, t):
        return remote(at(i, r, t), after(i, r, t), ag_send.at[i, r, t % 2], ag_recv.at[i, r, t % 2], r)

    for i, r in items:
        send(i, r, n - 2).wait_recv()
        load(i, r, n - 1).wait()
        here, there = own[i].at[r, (n - 1) % 2], got[i].at[r, (n - 2) % 2]
        for copy in state[i * RINGS + r]:
            copy.wait()
        wr, mr, vr = passed(out, slots, i, r ^ 1, 1), split(mo[i], i, r, 0), split(vo[i], i, r, 0)

        def update(rows, columns):
            at = (rows, columns)
            total = (here[at].astype(jnp.float32) + there[at].astype(jnp.float32)).astype(jnp.bfloat16)
            wr[at], mr[at], vr[at] = adamw(wr[at].astype(jnp.float32), mr[at], vr[at], total.astype(jnp.float32))

        tiles(*here.shape, update)
        forward(i, r, 0).start()
        send(i, r, n - 2).wait_send()

    def gather_step(t, credited=True):
        for i, r in items:
            forward(i, r, t - 1).wait_recv()
            if credited:
                credit(ag_free.at[i, r], r)

            @pl.when(t > 1)
            def _():
                pl.semaphore_wait(ag_free.at[i, r], 1)
                forward(i, r, t - 2).wait_send()

            forward(i, r, t).start()
        return 0

    lax.fori_loop(1, near, lambda t, _: gather_step(t), 0)
    for t in range(near, last):
        gather_step(t, credited=t < last - 1)
    for i, r in items:
        forward(i, r, last - 1).wait_recv()
        forward(i, r, last - 2).wait_send()
        forward(i, r, last - 1).wait_send()


def spread(n, k, slots, wc, out, got, own, m, v, wo, mo, vo, buf, sems):
    read_sem, write_sem, kept_sem, back_sem = sems
    me = lax.axis_index("dp")
    place = [position(me, r // 2, k) for r in range(RINGS)]
    items = [(i, r) for i in range(len(wc)) for r in range(RINGS)]
    last = n - HELD - 1
    near = last - 5

    def part(ref, i, r, t):
        return cut(ref, buf[i].shape[-2:], r, device((place[r] - WAYS[r] * t + n) % n, r // 2, k))

    def read(i, r, t):
        return pltpu.make_async_copy(part(wc[i], i, r, t), buf[i].at[r, t % DEPTH], read_sem.at[i, r, t % DEPTH])

    def write(i, r, t):
        return pltpu.make_async_copy(buf[i].at[r, t % DEPTH], part(wo[i], i, r, t), write_sem.at[i, r, t % DEPTH])

    straight = []
    for j, t in enumerate((0, *range(near + 1, last + 1))):
        for i, r in items:
            chunk = kept(out, got, own, slots, i, r, t, last)
            straight.append(pltpu.make_async_copy(chunk, part(wo[i], i, r, t), kept_sem.at[j, i, r]))
    for j, (source, target) in enumerate(((m, mo), (v, vo))):
        straight += [pltpu.make_async_copy(source[i], target[i], back_sem.at[j, i]) for i in range(len(source))]
    each = -(-len(straight) // near)

    for t in range(1, near + 2):
        if t <= near:
            for i, r in items:
                if t > DEPTH:
                    write(i, r, t - DEPTH).wait()
                read(i, r, t).start()
            for copy in straight[(t - 1) * each : t * each]:
                copy.start()
        if t > 1:
            for i, r in items:
                read(i, r, t - 1).wait()
                write(i, r, t - 1).start()
    for t in range(near - DEPTH + 1, near + 1):
        for i, r in items:
            write(i, r, t).wait()
    for copy in straight:
        copy.wait()


def fill(n, k, part, hops, wo, sem):
    me = lax.axis_index("dp")
    place = [position(me, r // 2, k) for r in range(RINGS)]
    writes = []
    for slot, ref in enumerate(wo):
        for r in range(RINGS):
            for which, at in enumerate((place[r] + WAYS[r] * HELD, place[r] - WAYS[r])):
                target = cut(ref, part, r ^ which, device((at + n) % n, r // 2, k))
                writes.append(pltpu.make_async_copy(hops[r].at[which, slot], target, sem.at[slot, r, which]))
    for one in writes:
        one.start()
    for one in writes:
        one.wait()


def sets(refs, *sizes):
    found, at = [], 0
    for size in sizes:
        found.append(refs[at : at + size])
        at += size
    return *found, refs[at:]


def solution(mesh):
    n = mesh.shape["dp"]
    k = math.isqrt(n)
    routes = []
    for r in range(RINGS):
        routes.append([(device(p, r // 2, k), device((p + WAYS[r]) % n, r // 2, k)) for p in range(n)])

    def step(*arrays):
        g, w, m, v = (arrays[i : i + 3] for i in (0, 3, 6, 9))
        count, bf16, f32 = len(g), jnp.bfloat16, jnp.float32
        parts = []
        for one in m:
            _, rows, columns = one.shape
            parts.append((rows // 2, columns) if rows // 2 % 8 == 0 else (rows, columns // 2))
        kinds = sorted(set(parts))
        slots = [(kinds.index(p), parts[:i].count(p)) for i, p in enumerate(parts)]
        groups = len(kinds)
        many = RINGS * groups

        hbm, vmem = pl.BlockSpec(memory_space=pl.ANY), pl.BlockSpec(memory_space=pltpu.VMEM)
        dma, plain = pltpu.SemaphoreType.DMA, pltpu.SemaphoreType.REGULAR
        both, one = (count, RINGS, 2), (count, RINGS)

        def by_ring(refs):
            return [refs[i : i + groups] for i in range(0, len(refs), groups)]

        def placed(values, space):
            return [pltpu.with_memory_space_constraint(a, space) for a in values]

        def rings(*refs):
            *ahead, out, got, own, sems = sets(refs, *[count] * 7, many, count, count)
            kernel(n, k, slots, *ahead, by_ring(out), got, own, sems)

        whole = [jax.ShapeDtypeStruct(a.shape, bf16) for a in w]
        moments = [pltpu.VMEM(a.shape, f32) for a in (*m, *v)]
        passing = [pltpu.VMEM((2, parts.count(p), *p), bf16) for _ in range(RINGS) for p in kinds]
        buffers = [pltpu.VMEM((RINGS, 2, *p), bf16) for p in parts * 2]
        made = pl.pallas_call(
            rings,
            out_shape=whole + moments + passing + buffers,
            in_specs=[hbm] * (4 * count),
            out_specs=[hbm] * count + [vmem] * (4 * count + many),
            scratch_shapes=[dma(both), dma(both), dma(both), plain(one), dma((3, *one)), dma(both), dma(both), plain(one)],
            compiler_params=pltpu.CompilerParams(
                collective_id=0, has_side_effects=True, vmem_limit_bytes=4 * 2**20
            ),
            name="rings",
        )(*placed((*g, *w, *m, *v), pltpu.HBM))
        gathered, moved, out, kept_here, _ = sets(made, count, 2 * count, many, 2 * count)
        hops = [lax.ppermute(a, "dp", routes[j // groups]) for j, a in enumerate(out)]

        def copies(*refs):
            wc, out, got, own, ms, vs, wo, mo, vo, buf, sems = sets(refs, count, many, *[count] * 8)
            spread(n, k, slots, wc, by_ring(out), got, own, ms, vs, wo, mo, vo, buf, sems)

        deep = (count, RINGS, DEPTH)
        final = pl.pallas_call(
            copies,
            out_shape=whole + [jax.ShapeDtypeStruct(a.shape, f32) for a in (*m, *v)],
            in_specs=[hbm] * count + [vmem] * (4 * count + many),
            out_specs=[hbm] * (3 * count),
            scratch_shapes=[pltpu.VMEM((RINGS, DEPTH, *p), bf16) for p in parts]
            + [dma(deep), dma(deep), dma((6, *one)), dma((2, count))],
            compiler_params=pltpu.CompilerParams(vmem_limit_bytes=9 * 2**20),
            cost_estimate=pl.CostEstimate(flops=10**9, bytes_accessed=112 * 10**6, transcendentals=0),
            name="spread",
        )(*gathered, *placed((*out, *kept_here, *moved), pltpu.VMEM))

        new, before = list(final[:count]), []
        for group, part in enumerate(kinds):
            its = [i for i, (one, _) in enumerate(slots) if one == group]

            def puts(*refs, part=part, size=len(its)):
                hops, _, wo, (sem,) = sets(refs, RINGS, len(refs) - RINGS - size - 1, size)
                fill(n, k, part, hops, wo, sem)

            filled = pl.pallas_call(
                puts,
                out_shape=[whole[i] for i in its],
                in_specs=[vmem] * RINGS + [hbm] * (len(its) + len(before)),
                out_specs=[hbm] * len(its),
                input_output_aliases={RINGS + j: j for j in range(len(its))},
                scratch_shapes=[dma((len(its), RINGS, 2))],
                compiler_params=pltpu.CompilerParams(vmem_limit_bytes=2 * 2**20),
                cost_estimate=pl.CostEstimate(flops=10**8, bytes_accessed=9 * 10**6, transcendentals=0),
                name=f"fill_{group}",
            )(*placed(hops[group::groups], pltpu.VMEM), *placed([*[final[i] for i in its], *before], pltpu.HBM))
            for i, one in zip(its, filled, strict=True):
                new[i] = one
            before = filled
        return (*new, *final[count:])

    all_of, block = P(None, None, None), P(None, "dp", None)
    return jax.shard_map(
        step,
        mesh=mesh,
        in_specs=(P(("rep", "dp"), None, None, None),) * 3 + (all_of,) * 3 + (block,) * 6,
        out_specs=(P("rep", None, None),) * 3 + (P("rep", "dp", None),) * 6,
        check_vma=False,
    )
```
